256 devices in a mesh: sy: 16 (over y, x), sx: 8 (over z), wl: 2 (over core).
Axes of the slice: x: 4, y: 4, z: 8, core: 2. Of those that a mesh axis runs over, the one named last changes fastest.
Arguments:
- interface_map: bfloat16 [32, 8, 1536, 2, 1536], P(('wl', 'sy'), 'sx'), parts along dimension 0, may hold values from -0.0625 to 0.0625
- source_trace: float32 [32, 8, 2, 64, 4, 384], P(('wl', 'sy'), 'sx'), parts along dimension 0, may hold values from -6 to 6
- restriction: float32 [32, 8, 2, 32, 4, 384], P(('wl', 'sy'), 'sx'), parts along dimension 0, may hold values from -0.009765625 to 0.009765625
- prolongation: float32 [32, 8, 2, 32, 4, 384], P(('wl', 'sy'), 'sx'), parts along dimension 0, may hold values from -0.109375 to 0.109375
- coarse_inverse: float32 [4, 32, 32], P('wl'), parts along dimension 0, may hold values from -0.75 to 0.75
Outputs:
- traces: float32 [32, 8, 2, 64, 4, 384], P(('wl', 'sy'), 'sx'), parts along dimension 0
- coarse_coef: float32 [4, 64, 32], P('wl'), parts along dimension 0
The draws below stay inside these ranges and needn't reach their ends.
There are 2 independent parts, one for each index of `wl`. The reference program is written for one: setup_inputs(seed, part) draws one part's arguments, and reference() takes and returns one part's arrays. A program takes and returns all parts, laid end to end along the dimension named above; each array names one. Nothing has to cross between parts.
All inputs are finite; a program needn't handle non-finite values.
Results may differ from the reference program's by a relative error of at most 0.0025.
Values sent between devices are 32-bit elements; how exact they have to be, the bound alone decides.
No kernel may reach another device: no remote copies, remote signals or barrier semaphores. Data moves between devices by JAX's collectives and lax.ppermute only.
A program may use at most 128 MiB of HBM per device.

```python
import jax
import jax.numpy as jnp
from jax import lax

M = 384
NC = 32
S = 64
ITERS = 6
SUBY = 16
SUBX = 8


def steps_of(stream_key, extent, cuts, low, top_value):
    loudness, own = 1.0, jax.random.fold_in(stream_key, 6)
    for position, parts in cuts:
        draws = jnp.exp(jax.random.uniform(jax.random.fold_in(own, position), (parts,), jnp.float32, low / len(cuts), top_value / len(cuts)))
        loudness = loudness * jnp.repeat(draws, extent[position] // parts).reshape([-1 if axis == position else 1 for axis in range(len(extent))])
    return loudness


def centred(key, extent, width, most, cuts=(), dtype=jnp.bfloat16):
    drawn = jax.random.normal(key, extent, jnp.float32) * width
    if len(cuts) > 0:
        drawn = steps_of(key, extent, cuts, -0.22, 0.18) * drawn
    return jnp.clip(drawn, min=-most, max=most).astype(dtype)


def setup_inputs(seed: int = 0, part: int = 0) -> dict:
    key_list = jax.random.split(jax.random.key(seed), 6)
    own_keys = jax.random.split(jax.random.fold_in(key_list[5], part), 6)
    return {
        "interface_map": centred(own_keys[0], (SUBY, SUBX, 4 * M, 2, 4 * M), (24 * M) ** -0.5, 0.0625, ((0, 16), (1, 8))),
        "source_trace": centred(own_keys[1], (SUBY, SUBX, 2, S, 4, M), 1.0, 6.0, ((0, 16), (1, 8)), jnp.float32),
        "restriction": centred(own_keys[2], (SUBY, SUBX, 2, NC, 4, M), (8 * M * SUBY * SUBX) ** -0.5, 0.009765625, ((0, 16), (1, 8)), jnp.float32),
        "prolongation": centred(own_keys[3], (SUBY, SUBX, 2, NC, 4, M), (96 * NC) ** -0.5, 0.109375, ((0, 16), (1, 8)), jnp.float32),
        "coarse_inverse": centred(own_keys[4], (2, NC, NC), (2 * NC) ** -0.5, 0.75, (), jnp.float32),
    }


PRECISE = lax.Precision.HIGHEST


def shifted(values, along, offset):
    length_axis = values.shape[along]
    blank_edge = jnp.zeros_like(lax.slice_in_dim(values, 0, 1, axis=along))
    if offset == 1:
        return jnp.concatenate([blank_edge, lax.slice_in_dim(values, 0, length_axis - 1, axis=along)], axis=along)
    return jnp.concatenate([lax.slice_in_dim(values, 1, length_axis, axis=along), blank_edge], axis=along)


def complex_pair(left_real, left_imag, right_real, right_imag, pattern):
    real_part = jnp.einsum(pattern, left_real, right_real, precision=PRECISE) - jnp.einsum(pattern, left_imag, right_imag, precision=PRECISE)
    imag_part = jnp.einsum(pattern, left_real, right_imag, precision=PRECISE) + jnp.einsum(pattern, left_imag, right_real, precision=PRECISE)
    return jnp.stack([real_part, imag_part])


def corner_values(outgoing):
    corner_northwest = outgoing[..., 0, 0] + outgoing[..., 2, 0]
    corner_northeast = outgoing[..., 0, -1] + outgoing[..., 3, 0]
    corner_southwest = outgoing[..., 1, 0] + outgoing[..., 2, -1]
    corner_southeast = outgoing[..., 1, -1] + outgoing[..., 3, -1]
    return corner_northwest, corner_northeast, corner_southwest, corner_southeast


def assemble(from_north, from_south, from_west, from_east, into_northwest, into_northeast, into_southwest, into_southeast):
    north_side = from_north.at[..., 0].add(0.5 * into_northwest).at[..., -1].add(0.5 * into_northeast)
    south_side = from_south.at[..., 0].add(0.5 * into_southwest).at[..., -1].add(0.5 * into_southeast)
    west_side = from_west.at[..., 0].add(0.5 * into_northwest).at[..., -1].add(0.5 * into_southwest)
    east_side = from_east.at[..., 0].add(0.5 * into_northeast).at[..., -1].add(0.5 * into_southeast)
    return jnp.stack([north_side, south_side, west_side, east_side], axis=-2)


def reference(interface_map, source_trace, restriction, prolongation, coarse_inverse):
    grid_rows, grid_cols = source_trace.shape[0], source_trace.shape[1]
    src_count, side_len = source_trace.shape[3], source_trace.shape[5]
    coarse_width = restriction.shape[3]
    flat_map = interface_map.reshape(grid_rows * grid_cols, 4 * side_len, 8 * side_len)
    rest_flat = restriction.reshape(grid_rows, grid_cols, 2, coarse_width, 4 * side_len)
    lift_flat = prolongation.reshape(grid_rows, grid_cols, 2, coarse_width, 4 * side_len)
    traces = jnp.zeros(source_trace.shape, jnp.float32)
    coef_now = jnp.zeros((2, src_count, coarse_width), jnp.float32)
    for sweep_index in range(ITERS):
        flat_traces = traces.reshape(grid_rows, grid_cols, 2, src_count, 4 * side_len)
        coarse_total = complex_pair(flat_traces[:, :, 0], flat_traces[:, :, 1], rest_flat[:, :, 0], rest_flat[:, :, 1], "yxsk,yxnk->sn")
        coef_now = complex_pair(coarse_total[0], coarse_total[1], coarse_inverse[0], coarse_inverse[1], "sn,nq->sq")
        spread = complex_pair(coef_now[0], coef_now[1], lift_flat[:, :, 0], lift_flat[:, :, 1], "sn,yxnk->yxsk")
        corrected = flat_traces + jnp.moveaxis(spread, 0, 2)
        row_block = corrected.astype(jnp.bfloat16).reshape(grid_rows * grid_cols, 2 * src_count, 4 * side_len)
        product = lax.map(lambda operands: jnp.dot(operands[0], operands[1], preferred_element_type=jnp.float32), (row_block, flat_map))
        product = product.reshape(grid_rows, grid_cols, 2, src_count, 2, 4 * side_len)
        real_part = product[:, :, 0, :, 0] - product[:, :, 1, :, 1]
        imag_part = product[:, :, 0, :, 1] + product[:, :, 1, :, 0]
        outgoing = jnp.stack([real_part, imag_part], axis=2).reshape(source_trace.shape) + source_trace
        from_north = shifted(outgoing[:, :, :, :, 1], 0, 1)
        from_south = shifted(outgoing[:, :, :, :, 0], 0, -1)
        from_west = shifted(outgoing[:, :, :, :, 3], 1, 1)
        from_east = shifted(outgoing[:, :, :, :, 2], 1, -1)
        corner_northwest, corner_northeast, corner_southwest, corner_southeast = corner_values(outgoing)
        into_northwest = shifted(shifted(corner_southeast, 0, 1), 1, 1)
        into_northeast = shifted(shifted(corner_southwest, 0, 1), 1, -1)
        into_southwest = shifted(shifted(corner_northeast, 0, -1), 1, 1)
        into_southeast = shifted(shifted(corner_northwest, 0, -1), 1, -1)
        traces = assemble(from_north, from_south, from_west, from_east, into_northwest, into_northeast, into_southwest, into_southeast)
    return traces, coef_now
```

```python
import functools

import jax
import jax.numpy as jnp
from jax import lax
from jax.experimental import pallas as pl
from jax.experimental.pallas import tpu as pltpu
from jax.sharding import Mesh
from jax.sharding import PartitionSpec as P

ITERS = 6
SY = ("sy_0", "sy_1")
WL_SY = ("wl", "sy_0", "sy_1")
HIGHEST = lax.Precision.HIGHEST
NT = (((1,), (1,)), ((), ()))


def ring(value, axis, by):
    n = lax.axis_size(axis)
    return lax.ppermute(value, axis, [(i, (i + by) % n) for i in range(n)])


def exchange(north, south, west, east):
    from_west = ring(east, "sx", 1)
    from_east = ring(west, "sx", -1)
    from_north = ring(south, SY, 1)
    from_south = ring(north, SY, -1)
    rows = north.shape[0]
    relay = from_west[rows:] + from_east[rows:]
    relay_north = ring(relay, SY, 1)
    relay_south = ring(relay, SY, -1)
    return (from_north, from_south, from_west, from_east, relay_north, relay_south)


def butterfly_sum(value):
    for axis in ("sx", "sy_1", "sy_0"):
        n = lax.axis_size(axis)
        step = 1
        while step < n:
            value = value + lax.ppermute(value, axis, [(i, i ^ step) for i in range(n)])
            step *= 2
    return value


def lane(shape):
    return lax.broadcasted_iota(jnp.int32, shape, 1)


def sublane(shape):
    return lax.broadcasted_iota(jnp.int32, shape, 0)


def write_corners(rows, north, south, west, east, to_west, to_east):
    end = north.shape[1]
    first = lambda ref: ref[:rows, 0:1]
    last = lambda ref: ref[:rows, end - 1 : end]
    corner_nw = first(north) + first(west)
    corner_ne = last(north) + first(east)
    corner_sw = first(south) + last(west)
    corner_se = last(south) + last(east)
    at = lane((rows, 128))
    zero = jnp.zeros((rows, 128), jnp.float32)
    table = jnp.where(at == 0, corner_se, zero)
    table = jnp.where(at == 1, corner_sw, table)
    table = jnp.where(at == 4, corner_ne, table)
    table = jnp.where(at == 5, corner_nw, table)
    turned = table.T[:8]
    row = sublane((8, rows))
    to_east[rows:, :] = jnp.zeros((8, end), jnp.float32)
    to_west[rows:, :] = jnp.zeros((8, end), jnp.float32)
    to_east[rows:, :rows] = jnp.where(row % 4 == 0, turned, 0.0)
    to_west[rows:, :rows] = jnp.where(row % 4 == 1, turned, 0.0)


def place():
    sy = lax.axis_index("sy_0") * lax.axis_size("sy_1") + lax.axis_index("sy_1")
    sx = lax.axis_index("sx")
    return (
        sy > 0,
        sy < lax.axis_size("sy_0") * lax.axis_size("sy_1") - 1,
        sx > 0,
        sx < lax.axis_size("sx") - 1,
    )


def keep(cond, value):
    return jnp.where(cond, value, jnp.zeros_like(value))


def incoming(refs):
    from_north, from_south, from_west, from_east, relay_north, relay_south = refs
    rows, end = from_north.shape
    has_north, has_south, has_west, has_east = place()
    row = sublane((8, 256))
    mixed = jnp.where(row < 4, relay_north[:, :256], relay_south[:, :256])
    mixed = jnp.concatenate([mixed, jnp.zeros((120, 256), jnp.float32)], axis=0)
    turned = 0.5 * mixed.T[:rows]
    into_nw = keep(jnp.logical_and(has_north, has_west), turned[:, 0:1])
    into_ne = keep(jnp.logical_and(has_north, has_east), turned[:, 1:2])
    into_sw = keep(jnp.logical_and(has_south, has_west), turned[:, 4:5])
    into_se = keep(jnp.logical_and(has_south, has_east), turned[:, 5:6])
    at = lane((rows, end))

    def side(ref, has, at_first, at_last):
        value = keep(has, ref[:rows, :])
        return value + jnp.where(at == 0, at_first, jnp.where(at == end - 1, at_last, 0.0))

    return (
        side(from_north, has_north, into_nw, into_ne),
        side(from_south, has_south, into_sw, into_se),
        side(from_west, has_west, into_nw, into_sw),
        side(from_east, has_east, into_ne, into_se),
    )


def first_kernel(src, weights, north, south, west, east):
    n_src, n_coarse = src.shape[2], weights.shape[2]
    half = n_src + n_coarse
    for side, ref in enumerate((north, south, west, east)):
        for part in range(2):
            ref[part * half : part * half + n_src, :] = src[side, part]
            ref[part * half + n_src : (part + 1) * half, :] = weights[side, part]
    write_corners(2 * half, north, south, west, east, west, east)


def round_kernel(first, *refs):
    if first:
        *arrived, lift, table, src, north, south, west, east, extra, block, turned = refs
    else:
        *arrived, table, src, north, south, west, east, extra, block, turned = refs
    step = pl.program_id(0)
    n_src = src.shape[2]
    rows, end = arrived[0].shape
    half = rows // 2
    n_coarse = half - n_src

    @pl.when(step == 0)
    def _():
        for side, value in enumerate(incoming(arrived)):
            cols = slice(side * end, (side + 1) * end)
            for part in range(2):
                base = part * half
                extra[part * n_coarse : (part + 1) * n_coarse, cols] = value[base + n_src : base + half]
                low = value[base : base + n_src].astype(jnp.bfloat16)
                if first:
                    high = lift[part * n_coarse : (part + 1) * n_coarse, cols].astype(jnp.bfloat16)
                else:
                    high = value[base + n_src : base + half].astype(jnp.bfloat16)
                both = jnp.concatenate([low, high], axis=0)
                block[base : base + half, cols] = both
                turned[half - base : 2 * half - base, cols] = both if part == 0 else -both

    out = jnp.dot(block[...], table[0], preferred_element_type=jnp.float32) + jnp.dot(
        turned[...], table[1], preferred_element_type=jnp.float32
    )
    for side, ref in enumerate((north, south, west, east)):

        @pl.when(step == side)
        def _():
            for part in range(2):
                base = part * half
                ref[base : base + n_src, :] = out[base : base + n_src] + src[0, part]
                ref[base + n_src : base + half, :] = out[base + n_src : base + half]

    @pl.when(step == 3)
    def _():
        write_corners(rows, north, south, west, east, west, east)


def total_kernel(north, south, west, east, weights, total):
    rows, end = north.shape
    half = rows // 2
    acc = jnp.zeros((rows, 128), jnp.float32)
    for side, ref in enumerate((north, south, west, east)):
        part = weights[:, side * end : (side + 1) * end]
        acc += lax.dot_general(
            ref[:rows, :],
            jnp.concatenate([part, part], axis=0),
            NT,
            precision=HIGHEST,
            preferred_element_type=jnp.float32,
        )
    swapped = pltpu.roll(acc[half:], 32, 1)
    total[...] = acc[:half] + jnp.where(lane((half, 128)) % 64 < 32, -swapped, swapped)


def coef_kernel(first_total, sums, inverse, coef):
    n_src = first_total.shape[0]
    n_coarse = inverse.shape[0]

    def times(value):
        sign = lane((n_coarse, 128)) % 64 < 32
        moved = pltpu.roll(value, 32, 1)
        lower = jnp.where(sign, -moved, moved)
        return jnp.concatenate([value, lower, jnp.zeros((128 - 2 * n_coarse, 128), jnp.float32)], axis=0)

    dot = functools.partial(jnp.dot, precision=HIGHEST, preferred_element_type=jnp.float32)
    by_inverse = times(inverse[...])
    steps = sums.shape[0] // (n_src + n_coarse)
    moves = []
    totals = [first_total[...]]
    for i in range(steps):
        base = i * (n_src + n_coarse)
        totals.append(sums[base : base + n_src, :])
        moves.append(times(sums[base + n_src : base + n_src + n_coarse, :]))
    coefs = []
    for i, value in enumerate(totals):
        for j in range(i):
            value = value + dot(coefs[j], moves[i - j - 1])
        coefs.append(dot(value, by_inverse))
    for i, value in enumerate(coefs):
        coef[i] = value


def last_kernel(n_src, *refs):
    *arrived, v1, v2, v3, v4, coef, out = refs
    rows, end = arrived[0].shape
    half = rows // 2
    sides = incoming(arrived)
    lefts = []
    for j in range(5):
        value = coef[j]
        at = lane(value.shape) % 64 < 32
        lefts.append(
            jnp.concatenate([jnp.where(at, value, -value), pltpu.roll(value, 32, 1)], axis=0)[:, :64]
        )
    for side, value in enumerate(sides):
        cols = slice(side * end, (side + 1) * end)
        moved = jnp.concatenate([value[n_src:half], value[half + n_src :]], axis=0)
        acc = jnp.concatenate([value[:n_src], value[half : half + n_src]], axis=0)
        for j, moved_j in enumerate((moved, v4[:, cols], v3[:, cols], v2[:, cols], v1[:, cols])):
            acc += jnp.dot(lefts[j], moved_j, precision=HIGHEST, preferred_element_type=jnp.float32)
        out[side, 0] = acc[:n_src]
        out[side, 1] = acc[n_src:]


def whole(x):
    return pl.BlockSpec(x.shape, lambda *_: (0,) * len(x.shape))


def per_device(interface_map, source_trace, restriction, prolongation, coarse_inverse):
    _, n_src, _, end = source_trace.shape[2:]
    n_coarse = restriction.shape[3]
    half = n_src + n_coarse
    rows = 2 * half
    f32 = jnp.float32
    src = jnp.moveaxis(source_trace[0, 0], 2, 0)
    weights = jnp.moveaxis(restriction[0, 0], 2, 0)
    lift = prolongation[0, 0].reshape(2 * n_coarse, 4 * end)
    table = jnp.moveaxis(interface_map[0, 0], 1, 0)
    side = jax.ShapeDtypeStruct((rows, end), f32)
    long_side = jax.ShapeDtypeStruct((rows + 8, end), f32)
    params = pltpu.CompilerParams(vmem_limit_bytes=32 * 1024 * 1024)

    sent = pl.pallas_call(
        first_kernel, out_shape=(side, side, long_side, long_side), compiler_params=params, name="first"
    )(src, weights)
    first_row = None
    weights_out = None
    kept = []
    sums = []
    inverse = jnp.concatenate([coarse_inverse[0], coarse_inverse[1]] * 2, axis=1)
    for i in range(1, ITERS):
        arrived = exchange(*sent)
        first = i == 1
        operands = [*arrived] + ([lift] if first else []) + [table, src]
        in_specs = [whole(x) for x in operands]
        in_specs[-2] = pl.BlockSpec((2, 4 * end, end), lambda s: (0, 0, s))
        in_specs[-1] = pl.BlockSpec((1, 2, n_src, end), lambda s: (s, 0, 0, 0))
        extra_shape = jax.ShapeDtypeStruct((2 * n_coarse, 4 * end), f32)
        outs = (side, side, long_side, long_side, extra_shape)
        *new_sent, extra = pl.pallas_call(
            functools.partial(round_kernel, first),
            grid=(4,),
            in_specs=in_specs,
            out_specs=tuple(whole(x) for x in outs),
            out_shape=outs,
            scratch_shapes=[pltpu.VMEM((rows, 4 * end), jnp.bfloat16)] * 2,
            compiler_params=params,
            cost_estimate=pl.CostEstimate(
                flops=2 * rows * 4 * end * 8 * end, bytes_accessed=12_000_000, transcendentals=0
            ),
            name="round",
        )(*operands)
        if first:
            weights_out = extra
            first_row = total(sent, weights_out, params)[:n_src]
        else:
            kept.append(extra)
        sent = new_sent
        if i < ITERS - 1:
            sums.append(total(sent, weights_out, params))
    arrived = exchange(*sent)
    reduced = butterfly_sum(jnp.concatenate([first_row, *sums], axis=0))
    coef = pl.pallas_call(
        coef_kernel,
        out_shape=jax.ShapeDtypeStruct((ITERS - 1, n_src, 128), f32),
        compiler_params=params,
        name="coef",
    )(reduced[:n_src], reduced[n_src:], inverse)
    traces = pl.pallas_call(
        functools.partial(last_kernel, n_src),
        out_shape=jax.ShapeDtypeStruct((4, 2, n_src, end), f32),
        compiler_params=params,
        name="last",
    )(*arrived, *kept, coef)
    traces = jnp.moveaxis(traces, 0, 2)
    final = coef[ITERS - 2]
    coef_now = jnp.stack([final[:, :n_coarse], final[:, n_coarse : 2 * n_coarse]])
    return (traces[None, None], coef_now)


def total(sent, weights, params):
    rows = sent[0].shape[0]
    return pl.pallas_call(
        total_kernel,
        out_shape=jax.ShapeDtypeStruct((rows // 2, 128), jnp.float32),
        compiler_params=params,
        cost_estimate=pl.CostEstimate(flops=300_000_000, bytes_accessed=1_600_000, transcendentals=0),
        name="total",
    )(*sent, weights)


def solution(mesh):
    finer = Mesh(
        mesh.devices.reshape(4, 4, mesh.shape["sx"], mesh.shape["wl"]), ("sy_0", "sy_1", "sx", "wl")
    )
    return jax.shard_map(
        per_device,
        mesh=finer,
        in_specs=(
            P(WL_SY, "sx", None, None, None),
            P(WL_SY, "sx", None, None, None, None),
            P(WL_SY, "sx", None, None, None, None),
            P(WL_SY, "sx", None, None, None, None),
            P("wl", None, None),
        ),
        out_specs=(P(WL_SY, "sx", None, None, None, None), P("wl", None, None)),
        check_vma=False,
    )
```

```python
import functools

import jax
import jax.numpy as jnp
from jax import lax
from jax.experimental import pallas as pl
from jax.experimental.pallas import tpu as pltpu
from jax.sharding import Mesh
from jax.sharding import PartitionSpec as P


ITERS = 6
SY = ("sy_0", "sy_1")
WL_SY = ("wl", "sy_0", "sy_1")
HIGHEST = lax.Precision.HIGHEST
TILE = 512
NT = (((1,), (1,)), ((), ()))
SUM_STEPS = (("sx", (4,)), ("sx", (1, 2, 3)), ("sy_1", (1, 2, 3)), ("sy_0", (1, 2, 3)))


def ring(value, axis, by):
    n = lax.axis_size(axis)
    return lax.ppermute(value, axis, [(i, (i + by) % n) for i in range(n)])


def exchange(north, south, west, east):
    from_west = ring(east, "sx", 1)
    from_east = ring(west, "sx", -1)
    from_north = ring(south, SY, 1)
    from_south = ring(north, SY, -1)
    rows = north.shape[0]
    relay = from_west[rows:] + from_east[rows:]
    relay_north = ring(relay, SY, 1)
    relay_south = ring(relay, SY, -1)
    return (from_north, from_south, from_west, from_east, relay_north, relay_south)


def butterfly_sum(value):
    for axis, partners in SUM_STEPS:
        n = lax.axis_size(axis)
        others = [lax.ppermute(value, axis, [(i, i ^ p) for i in range(n)]) for p in partners]
        value = functools.reduce(jnp.add, others, value)
    return value


def lane(shape):
    return lax.broadcasted_iota(jnp.int32, shape, 1)


def sublane(shape):
    return lax.broadcasted_iota(jnp.int32, shape, 0)


def write_corners(rows, north, south, west, east, to_west, to_east):
    end = north.shape[1]
    first = lambda ref: ref[:rows, 0:1]
    last = lambda ref: ref[:rows, end - 1 : end]
    corner_nw = first(north) + first(west)
    corner_ne = last(north) + first(east)
    corner_sw = first(south) + last(west)
    corner_se = last(south) + last(east)
    at = lane((rows, 128))
    zero = jnp.zeros((rows, 128), jnp.float32)
    table = jnp.where(at == 0, corner_se, zero)
    table = jnp.where(at == 1, corner_sw, table)
    table = jnp.where(at == 4, corner_ne, table)
    table = jnp.where(at == 5, corner_nw, table)
    turned = table.T[:8]
    row = sublane((8, rows))
    to_east[rows:, :] = jnp.zeros((8, end), jnp.float32)
    to_west[rows:, :] = jnp.zeros((8, end), jnp.float32)
    to_east[rows:, :rows] = jnp.where(row % 4 == 0, turned, 0.0)
    to_west[rows:, :rows] = jnp.where(row % 4 == 1, turned, 0.0)


def place():
    sy = lax.axis_index("sy_0") * lax.axis_size("sy_1") + lax.axis_index("sy_1")
    sx = lax.axis_index("sx")
    return (
        sy > 0,
        sy < lax.axis_size("sy_0") * lax.axis_size("sy_1") - 1,
        sx > 0,
        sx < lax.axis_size("sx") - 1,
    )


def keep(cond, value):
    return jnp.where(cond, value, jnp.zeros_like(value))


def incoming(refs):
    from_north, from_south, from_west, from_east, relay_north, relay_south = refs
    rows, end = from_north.shape
    has_north, has_south, has_west, has_east = place()
    row = sublane((8, 256))
    mixed = jnp.where(row < 4, relay_north[:, :256], relay_south[:, :256])
    mixed = jnp.concatenate([mixed, jnp.zeros((120, 256), jnp.float32)], axis=0)
    turned = 0.5 * mixed.T[:rows]
    into_nw = keep(jnp.logical_and(has_north, has_west), turned[:, 0:1])
    into_ne = keep(jnp.logical_and(has_north, has_east), turned[:, 1:2])
    into_sw = keep(jnp.logical_and(has_south, has_west), turned[:, 4:5])
    into_se = keep(jnp.logical_and(has_south, has_east), turned[:, 5:6])
    at = lane((rows, end))

    def side(ref, has, at_first, at_last):
        value = keep(has, ref[:rows, :])
        return value + jnp.where(at == 0, at_first, jnp.where(at == end - 1, at_last, 0.0))

    return (
        side(from_north, has_north, into_nw, into_ne),
        side(from_south, has_south, into_sw, into_se),
        side(from_west, has_west, into_nw, into_sw),
        side(from_east, has_east, into_ne, into_se),
    )


def first_kernel(src, weights, north, south, west, east, whole_out):
    n_src, n_coarse = src.shape[1], weights.shape[1]
    half = n_src + n_coarse
    for side, ref in enumerate((north, south, west, east)):
        for part in range(2):
            ref[part * half : part * half + n_src, :] = src[part, :, side, :]
            ref[part * half + n_src : (part + 1) * half, :] = weights[part, :, side, :]
        whole_out[:, side * ref.shape[1] : (side + 1) * ref.shape[1]] = ref[: 2 * half, :]
    write_corners(2 * half, north, south, west, east, west, east)


def round_kernel(number, *refs):
    first, sends, receives, hides = number == 1, number == 2, number == 3, number > 3
    arrived, refs = refs[:6], list(refs[6:])
    lift = refs.pop(0) if first else None
    sent_along = refs.pop(0) if sends else None
    far = refs.pop(0) if first else None
    table = None if first else refs.pop(0)
    src, north, south, west, east, extra = refs[:6]
    rest = refs[6:]
    if hides:
        block, whole_out = rest
    elif first:
        whole_out, table, block, arrives = rest
    elif receives:
        whole_out, received, block = rest
    else:
        whole_out, block = rest
    end = arrived[0].shape[1]
    rows = whole_out.shape[0]
    half = rows // 2
    n_src = half - extra.shape[0] // 2
    count = 4 * end // TILE

    def bring(t):
        cols = pl.ds(pl.multiple_of(t * TILE, TILE), TILE)
        return pltpu.make_async_copy(far.at[:, :, cols], table.at[:, :, cols], arrives.at[t])

    if first:
        for t in range(count):
            bring(t).start()
    n_coarse = half - n_src
    row, col = sublane((256, 256)), lane((256, 256))
    weave = (row == col // 2 + 128 * (col % 2)).astype(jnp.bfloat16)
    for side, value in enumerate(incoming(arrived)):
        cols = slice(side * end, (side + 1) * end)
        if receives:
            received[:, cols] = value[rows:]
        plain = []
        for part in range(2):
            base = part * half
            extra[part * n_coarse : (part + 1) * n_coarse, cols] = value[base + n_src : base + half]
            low = value[base : base + n_src].astype(jnp.bfloat16)
            if first:
                high = lift[part, :, side, :].astype(jnp.bfloat16)
            else:
                high = value[base + n_src : base + half].astype(jnp.bfloat16)
            plain.append(jnp.concatenate([low, high], axis=0))
        straight = jnp.concatenate(plain, axis=0)
        turned = jnp.concatenate([-plain[1], plain[0]], axis=0)
        for k in range(0, end, 128):
            pair = jnp.concatenate([straight[:, k : k + 128], turned[:, k : k + 128]], axis=1)
            woven = jnp.dot(pair, weave, preferred_element_type=jnp.float32)
            block[:, 2 * (side * end + k) : 2 * (side * end + k) + 256] = woven.astype(jnp.bfloat16)

    def columns(t, carry):
        cols = pl.ds(pl.multiple_of(t * TILE, TILE), TILE)
        if first:
            bring(t).wait()
        whole_out[:, cols] = jnp.dot(
            block[...], table[:, :, cols].reshape(8 * end, TILE), preferred_element_type=jnp.float32
        )
        return carry

    lax.fori_loop(0, count, columns, 0)
    for side, ref in enumerate((north, south, west, east)):
        cols = slice(side * end, (side + 1) * end)
        for part in range(2):
            base = part * half
            value = whole_out[base : base + n_src, cols] + src[base : base + n_src, cols]
            ref[base : base + n_src, :] = value
            if not hides:
                whole_out[base : base + n_src, cols] = value
            ref[base + n_src : base + half, :] = whole_out[base + n_src : base + half, cols]
        if sends:
            ref[rows : north.shape[0], :] = sent_along[:, cols]
    write_corners(north.shape[0], north, south, west, east, west, east)


def adjoint_kernel(weights, table, out):
    n, length = weights.shape
    half = n // 2
    value = weights[...]
    high = value.astype(jnp.bfloat16)
    low = (value - high.astype(jnp.float32)).astype(jnp.bfloat16)
    left = jnp.concatenate([high, low], axis=0)
    row, col = sublane((256, 256)), lane((256, 256))
    unweave = (col == row // 2 + 128 * (row % 2)).astype(jnp.bfloat16)

    def some(t, carry):
        for k in range(3):
            here = pl.multiple_of(t * 384 + k * 128, 128)
            part = table[pl.ds(here, 128), :, :].reshape(256, length)
            both = lax.dot_general(left, part, NT, preferred_element_type=jnp.float32)
            both = both[:n] + both[n:]
            upper = both.astype(jnp.bfloat16)
            rest = both - upper.astype(jnp.float32)
            middle = rest.astype(jnp.bfloat16)
            lower = (rest - middle.astype(jnp.float32)).astype(jnp.bfloat16)
            split = jnp.concatenate([upper, middle, lower], axis=0)
            split = jnp.dot(split, unweave, preferred_element_type=jnp.float32)
            both = split[:n] + split[n : 2 * n] + split[2 * n :]
            out[:half, pl.ds(here, 128)] = both[:half, :128] - both[half:, 128:]
            out[half:, pl.ds(here, 128)] = both[:half, 128:] + both[half:, :128]
        return carry

    lax.fori_loop(0, length // 384, some, 0)


def total_kernel(out, left, right, total):
    rows, length = out.shape
    half = rows // 2

    def columns(t, acc):
        cols = pl.ds(pl.multiple_of(t * TILE, TILE), TILE)
        return acc + lax.dot_general(
            out[:, cols],
            jnp.concatenate([left[:, cols], right[:, cols]], axis=0),
            NT,
            precision=HIGHEST,
            preferred_element_type=jnp.float32,
        )

    acc = lax.fori_loop(0, length // TILE, columns, jnp.zeros((rows, 128), jnp.float32))
    at = lane((half, 128)) % 64 < 32
    ahead, behind = pltpu.roll(acc[half:], 96, 1), pltpu.roll(acc[half:], 32, 1)
    total[...] = acc[:half] + jnp.where(at, -ahead, behind)


def coef_kernel(n_src, sums, inverse, coef, final):
    n_coarse = inverse.shape[0]
    half = n_src + n_coarse

    def spread(value, upper):
        at = lane(value.shape) >= 64
        kept = jnp.where(at if upper else jnp.logical_not(at), value, 0.0)
        return kept + pltpu.roll(kept, 64, 1)

    def times(value):
        sign = lane((n_coarse, 128)) % 64 < 32
        moved = pltpu.roll(value, 32, 1)
        lower = jnp.where(sign, -moved, moved)
        return jnp.concatenate([value, lower, jnp.zeros((128 - 2 * n_coarse, 128), jnp.float32)], axis=0)

    dot = functools.partial(jnp.dot, precision=HIGHEST, preferred_element_type=jnp.float32)
    by_inverse = times(inverse[...])
    first, second = sums[:half, :], sums[half : 2 * half, :]
    folded = sums[2 * half :, :]
    one = jnp.concatenate([spread(folded, False), spread(folded, True)], axis=0)
    rest = [spread(first, False), spread(first, True), spread(second, False), spread(second, True)]
    totals = [one] + [value[:n_src] for value in rest]
    totals[-1] = totals[-1] + one
    moves = [times(value[n_src:]) for value in rest]
    coefs = []
    for i, value in enumerate(totals):
        for j in range(i):
            value = value + dot(coefs[j], moves[i - j - 1])
        coefs.append(dot(value, by_inverse))
    sign = lane((n_src, 128)) % 64 < 32
    for i, value in enumerate(coefs):
        coef[:n_src, i * 64 : (i + 1) * 64] = jnp.where(sign, value, -value)[:, :64]
        coef[n_src:, i * 64 : (i + 1) * 64] = pltpu.roll(value, 32, 1)[:, :64]
    final[0] = coefs[-1][:, :n_coarse]
    final[1] = coefs[-1][:, n_coarse : 2 * n_coarse]


def last_kernel(n_src, *refs):
    *arrived, v1, v2, v3, v4, coef, out, moved, acc = refs
    rows, end = arrived[0].shape
    half = rows // 2
    n_coarse = half - n_src
    for side, value in enumerate(incoming(arrived)):
        cols = slice(side * end, (side + 1) * end)
        for part in range(2):
            base = part * half
            acc[side, part * n_src : (part + 1) * n_src] = value[base : base + n_src]
            moved[part * n_coarse : (part + 1) * n_coarse, cols] = value[base + n_src : base + half]

    def one(side, carry):
        cols = pl.ds(pl.multiple_of(side * end, 128), end)
        right = jnp.concatenate([ref[:, cols] for ref in (moved, v4, v3, v2, v1)], axis=0)
        acc[side] += jnp.dot(coef[...], right, precision=HIGHEST, preferred_element_type=jnp.float32)
        return carry

    lax.fori_loop(0, 4, one, 0)
    for side in range(4):
        for part in range(2):
            out[part, :, side, :] = acc[side, part * n_src : (part + 1) * n_src]


def per_device(interface_map, source_trace, restriction, prolongation, coarse_inverse):
    _, n_src, _, end = source_trace.shape[2:]
    n_coarse = restriction.shape[3]
    half = n_src + n_coarse
    rows = 2 * half
    f32 = jnp.float32
    lift = prolongation[0, 0]
    table = interface_map[0, 0]
    side = jax.ShapeDtypeStruct((rows, end), f32)
    long_side = jax.ShapeDtypeStruct((rows + 8, end), f32)
    params = pltpu.CompilerParams(vmem_limit_bytes=32 * 1024 * 1024)

    wide = jax.ShapeDtypeStruct((rows, 4 * end), f32)
    *sent, out = pl.pallas_call(
        first_kernel, out_shape=(side, side, long_side, long_side, wide), compiler_params=params, name="first"
    )(source_trace[0, 0], restriction[0, 0])
    src = out
    kept = []
    outs = [out]
    wider = lambda shape: jax.ShapeDtypeStruct((shape.shape[0] + 2 * n_coarse, shape.shape[1]), f32)
    inverse = jnp.concatenate([coarse_inverse[0], coarse_inverse[1]] * 2, axis=1)
    extra_shape = jax.ShapeDtypeStruct((2 * n_coarse, 4 * end), f32)
    for i in range(1, ITERS):
        arrived = exchange(*sent)
        operands = [*arrived] + ([lift] if i == 1 else []) + ([adjoint] if i == 2 else []) + [table, src]
        sides = tuple(wider(x) if i == 2 else x for x in (side, side, long_side, long_side))
        more = {1: (wide, table), 2: (wide,), 3: (wide, extra_shape)}.get(i, ())
        scratch = [pltpu.VMEM((rows, 8 * end), jnp.bfloat16)]
        specs = [pl.BlockSpec(memory_space=pltpu.VMEM)] * len(operands)
        if i == 1:
            specs[-2] = pl.BlockSpec(memory_space=pl.ANY)
            scratch.append(pltpu.SemaphoreType.DMA((4 * end // TILE,)))
        if i > 3:
            scratch.append(pltpu.VMEM((rows, 4 * end), f32))
        out_shape = sides + (extra_shape,) + tuple(jax.ShapeDtypeStruct(x.shape, x.dtype) for x in more)
        results = pl.pallas_call(
            functools.partial(round_kernel, i),
            in_specs=specs,
            out_shape=out_shape,
            scratch_shapes=scratch,
            compiler_params=params,
            cost_estimate=pl.CostEstimate(
                flops=2 * rows * 4 * end * 8 * end, bytes_accessed=12_000_000, transcendentals=0
            ),
            name="round",
        )(*operands)
        sent, extra = results[:4], results[4]
        if i < 4:
            out = results[5]
            outs.append(out)
        if i == 1:
            table = results[6]
        if i == 1:
            seen = extra
            adjoint = pl.pallas_call(
                adjoint_kernel,
                out_shape=extra_shape,
                compiler_params=params,
                cost_estimate=pl.CostEstimate(
                    flops=2 * rows * 4 * end * 8 * end, bytes_accessed=12_000_000, transcendentals=0
                ),
                name="adjoint",
            )(seen, table)
        else:
            kept.append(extra)
        if i == 3:
            t1, t2, t3 = (total(outs[j], seen, seen, params) for j in range(3))
            t45 = total(out, seen, results[6], params)
            at = lane((half, 128)) < 64
            fold = n_src // 2
            folded = jnp.where(lane((fold, 128)) < 64, t1[:fold], t1[fold:n_src])
            sums = butterfly_sum(jnp.concatenate([jnp.where(at, t2, t3), t45, folded], axis=0))
    arrived = exchange(*sent)
    coef, coef_now = pl.pallas_call(
        functools.partial(coef_kernel, n_src),
        out_shape=(
            jax.ShapeDtypeStruct((2 * n_src, (ITERS - 1) * 64), f32),
            jax.ShapeDtypeStruct((2, n_src, n_coarse), f32),
        ),
        compiler_params=params,
        name="coef",
    )(sums, inverse)
    traces = pl.pallas_call(
        functools.partial(last_kernel, n_src),
        out_shape=jax.ShapeDtypeStruct((2, n_src, 4, end), f32),
        scratch_shapes=[pltpu.VMEM((2 * n_coarse, 4 * end), f32), pltpu.VMEM((4, 2 * n_src, end), f32)],
        compiler_params=params,
        name="last",
    )(*arrived, *kept, coef)
    return (traces[None, None], coef_now)


def total(out, left, right, params):
    return pl.pallas_call(
        total_kernel,
        out_shape=jax.ShapeDtypeStruct((out.shape[0] // 2, 128), jnp.float32),
        compiler_params=params,
        cost_estimate=pl.CostEstimate(flops=300_000_000, bytes_accessed=1_600_000, transcendentals=0),
        name="total",
    )(out, left, right)


def solution(mesh):
    finer = Mesh(
        mesh.devices.reshape(4, 4, mesh.shape["sx"], mesh.shape["wl"]), ("sy_0", "sy_1", "sx", "wl")
    )
    return jax.shard_map(
        per_device,
        mesh=finer,
        in_specs=(
            P(WL_SY, "sx", None, None, None),
            P(WL_SY, "sx", None, None, None, None),
            P(WL_SY, "sx", None, None, None, None),
            P(WL_SY, "sx", None, None, None, None),
            P("wl", None, None),
        ),
        out_specs=(P(WL_SY, "sx", None, None, None, None), P("wl", None, None)),
        check_vma=False,
    )
```

```python
import functools

import jax
import jax.numpy as jnp
from jax import lax
from jax.experimental import pallas as pl
from jax.experimental.pallas import tpu as pltpu
from jax.sharding import Mesh
from jax.sharding import PartitionSpec as P


ITERS = 6
SY = ("sy_0", "sy_1")
WL_SY = ("wl", "sy_0", "sy_1")
HIGHEST = lax.Precision.HIGHEST
TILE = 512
NT = (((1,), (1,)), ((), ()))
SUM_STEPS = (("sy_0", (1, 2, 3)), ("sy_1", (1, 2, 3)), ("sx", (1,)), ("sx", (2,)), ("sx", (4,)))


def ring(value, axis, by):
    n = lax.axis_size(axis)
    return lax.ppermute(value, axis, [(i, (i + by) % n) for i in range(n)])


def exchange(north, south, west, east):
    from_west = ring(east, "sx", 1)
    from_east = ring(west, "sx", -1)
    from_north = ring(south, SY, 1)
    from_south = ring(north, SY, -1)
    rows = north.shape[0]
    relay = from_west[rows:] + from_east[rows:]
    relay_north = ring(relay, SY, 1)
    relay_south = ring(relay, SY, -1)
    return (from_north, from_south, from_west, from_east, relay_north, relay_south)


def butterfly_sum(value):
    for axis, partners in SUM_STEPS:
        n = lax.axis_size(axis)
        others = [lax.ppermute(value, axis, [(i, i ^ p) for i in range(n)]) for p in partners]
        value = functools.reduce(jnp.add, others, value)
    return value


def lane(shape):
    return lax.broadcasted_iota(jnp.int32, shape, 1)


def sublane(shape):
    return lax.broadcasted_iota(jnp.int32, shape, 0)


def write_corners(rows, north, south, west, east, to_west, to_east):
    end = north.shape[1]
    first = lambda ref: ref[:rows, 0:1]
    last = lambda ref: ref[:rows, end - 1 : end]
    corner_nw = first(north) + first(west)
    corner_ne = last(north) + first(east)
    corner_sw = first(south) + last(west)
    corner_se = last(south) + last(east)
    at = lane((rows, 128))
    zero = jnp.zeros((rows, 128), jnp.float32)
    table = jnp.where(at == 0, corner_se, zero)
    table = jnp.where(at == 1, corner_sw, table)
    table = jnp.where(at == 4, corner_ne, table)
    table = jnp.where(at == 5, corner_nw, table)
    turned = table.T[:8]
    row = sublane((8, rows))
    to_east[rows:, :] = jnp.zeros((8, end), jnp.float32)
    to_west[rows:, :] = jnp.zeros((8, end), jnp.float32)
    to_east[rows:, :rows] = jnp.where(row % 4 == 0, turned, 0.0)
    to_west[rows:, :rows] = jnp.where(row % 4 == 1, turned, 0.0)


def place():
    sy = lax.axis_index("sy_0") * lax.axis_size("sy_1") + lax.axis_index("sy_1")
    sx = lax.axis_index("sx")
    return (
        sy > 0,
        sy < lax.axis_size("sy_0") * lax.axis_size("sy_1") - 1,
        sx > 0,
        sx < lax.axis_size("sx") - 1,
    )


def keep(cond, value):
    return jnp.where(cond, value, jnp.zeros_like(value))


def incoming(refs):
    from_north, from_south, from_west, from_east, relay_north, relay_south = refs
    rows, end = from_north.shape
    has_north, has_south, has_west, has_east = place()
    row = sublane((8, 256))
    mixed = jnp.where(row < 4, relay_north[:, :256], relay_south[:, :256])
    mixed = jnp.concatenate([mixed, jnp.zeros((120, 256), jnp.float32)], axis=0)
    turned = 0.5 * mixed.T[:rows]
    into_nw = keep(jnp.logical_and(has_north, has_west), turned[:, 0:1])
    into_ne = keep(jnp.logical_and(has_north, has_east), turned[:, 1:2])
    into_sw = keep(jnp.logical_and(has_south, has_west), turned[:, 4:5])
    into_se = keep(jnp.logical_and(has_south, has_east), turned[:, 5:6])
    at = lane((rows, end))

    def side(ref, has, at_first, at_last):
        value = keep(has, ref[:rows, :])
        return value + jnp.where(at == 0, at_first, jnp.where(at == end - 1, at_last, 0.0))

    return (
        side(from_north, has_north, into_nw, into_ne),
        side(from_south, has_south, into_sw, into_se),
        side(from_west, has_west, into_nw, into_sw),
        side(from_east, has_east, into_ne, into_se),
    )


def first_kernel(src, weights, north, south, west, east, whole_out):
    n_src, n_coarse = src.shape[1], weights.shape[1]
    half = n_src + n_coarse
    for side, ref in enumerate((north, south, west, east)):
        for part in range(2):
            ref[part * half : part * half + n_src, :] = src[part, :, side, :]
            ref[part * half + n_src : (part + 1) * half, :] = weights[part, :, side, :]
        whole_out[:, side * ref.shape[1] : (side + 1) * ref.shape[1]] = ref[: 2 * half, :]
    write_corners(2 * half, north, south, west, east, west, east)


def round_kernel(number, *refs):
    first, sends, receives, hides = number == 1, number == 2, number == 3, number > 3
    arrived, refs = refs[:6], list(refs[6:])
    lift = refs.pop(0) if first else None
    sent_along = refs.pop(0) if sends else None
    far = refs.pop(0) if first else None
    table = None if first else refs.pop(0)
    src, north, south, west, east, extra = refs[:6]
    rest = refs[6:]
    if hides:
        block, whole_out = rest
    elif first:
        whole_out, table, block, arrives = rest
    elif receives:
        whole_out, received, block = rest
    else:
        whole_out, block = rest
    end = arrived[0].shape[1]
    rows = whole_out.shape[0]
    half = rows // 2
    n_src = half - extra.shape[0] // 2
    count = 4 * end // TILE

    def bring(t):
        cols = pl.ds(pl.multiple_of(t * TILE, TILE), TILE)
        return pltpu.make_async_copy(far.at[:, :, cols], table.at[:, :, cols], arrives.at[t])

    if first:
        for t in range(count):
            bring(t).start()
    n_coarse = half - n_src
    row, col = sublane((256, 256)), lane((256, 256))
    weave = (row == col // 2 + 128 * (col % 2)).astype(jnp.bfloat16)
    for side, value in enumerate(incoming(arrived)):
        cols = slice(side * end, (side + 1) * end)
        if receives:
            received[:, cols] = value[rows:]
        plain = []
        for part in range(2):
            base = part * half
            extra[part * n_coarse : (part + 1) * n_coarse, cols] = value[base + n_src : base + half]
            low = value[base : base + n_src].astype(jnp.bfloat16)
            if first:
                high = lift[part, :, side, :].astype(jnp.bfloat16)
            else:
                high = value[base + n_src : base + half].astype(jnp.bfloat16)
            plain.append(jnp.concatenate([low, high], axis=0))
        straight = jnp.concatenate(plain, axis=0)
        turned = jnp.concatenate([-plain[1], plain[0]], axis=0)
        for k in range(0, end, 128):
            pair = jnp.concatenate([straight[:, k : k + 128], turned[:, k : k + 128]], axis=1)
            woven = jnp.dot(pair, weave, preferred_element_type=jnp.float32)
            block[:, 2 * (side * end + k) : 2 * (side * end + k) + 256] = woven.astype(jnp.bfloat16)

    def columns(t, carry):
        cols = pl.ds(pl.multiple_of(t * TILE, TILE), TILE)
        if first:
            bring(t).wait()
        whole_out[:, cols] = jnp.dot(
            block[...], table[:, :, cols].reshape(8 * end, TILE), preferred_element_type=jnp.float32
        )
        return carry

    lax.fori_loop(0, count, columns, 0)
    for side, ref in enumerate((north, south, west, east)):
        cols = slice(side * end, (side + 1) * end)
        for part in range(2):
            base = part * half
            value = whole_out[base : base + n_src, cols] + src[base : base + n_src, cols]
            ref[base : base + n_src, :] = value
            if not hides:
                whole_out[base : base + n_src, cols] = value
            ref[base + n_src : base + half, :] = whole_out[base + n_src : base + half, cols]
        if sends:
            ref[rows : north.shape[0], :] = sent_along[:, cols]
    write_corners(north.shape[0], north, south, west, east, west, east)


def adjoint_kernel(weights, table, out):
    n, length = weights.shape
    half = n // 2
    value = weights[...]
    high = value.astype(jnp.bfloat16)
    low = (value - high.astype(jnp.float32)).astype(jnp.bfloat16)
    left = jnp.concatenate([high, low], axis=0)
    row, col = sublane((256, 256)), lane((256, 256))
    unweave = (col == row // 2 + 128 * (row % 2)).astype(jnp.bfloat16)

    def some(t, carry):
        for k in range(3):
            here = pl.multiple_of(t * 384 + k * 128, 128)
            part = table[pl.ds(here, 128), :, :].reshape(256, length)
            both = lax.dot_general(left, part, NT, preferred_element_type=jnp.float32)
            both = both[:n] + both[n:]
            upper = both.astype(jnp.bfloat16)
            rest = both - upper.astype(jnp.float32)
            middle = rest.astype(jnp.bfloat16)
            lower = (rest - middle.astype(jnp.float32)).astype(jnp.bfloat16)
            split = jnp.concatenate([upper, middle, lower], axis=0)
            split = jnp.dot(split, unweave, preferred_element_type=jnp.float32)
            both = split[:n] + split[n : 2 * n] + split[2 * n :]
            out[:half, pl.ds(here, 128)] = both[:half, :128] - both[half:, 128:]
            out[half:, pl.ds(here, 128)] = both[:half, 128:] + both[half:, :128]
        return carry

    lax.fori_loop(0, length // 384, some, 0)


def total_kernel(out, left, right, total):
    rows, length = out.shape
    half = rows // 2

    def columns(t, acc):
        cols = pl.ds(pl.multiple_of(t * TILE, TILE), TILE)
        return acc + lax.dot_general(
            out[:, cols],
            jnp.concatenate([left[:, cols], right[:, cols]], axis=0),
            NT,
            precision=HIGHEST,
            preferred_element_type=jnp.float32,
        )

    acc = lax.fori_loop(0, length // TILE, columns, jnp.zeros((rows, 128), jnp.float32))
    at = lane((half, 128)) % 64 < 32
    ahead, behind = pltpu.roll(acc[half:], 96, 1), pltpu.roll(acc[half:], 32, 1)
    total[...] = acc[:half] + jnp.where(at, -ahead, behind)


def coef_kernel(n_src, sums, inverse, coef, final):
    n_coarse = inverse.shape[0]
    half = n_src + n_coarse

    def spread(value, upper):
        at = lane(value.shape) >= 64
        kept = jnp.where(at if upper else jnp.logical_not(at), value, 0.0)
        return kept + pltpu.roll(kept, 64, 1)

    def times(value):
        sign = lane((n_coarse, 128)) % 64 < 32
        moved = pltpu.roll(value, 32, 1)
        lower = jnp.where(sign, -moved, moved)
        return jnp.concatenate([value, lower, jnp.zeros((128 - 2 * n_coarse, 128), jnp.float32)], axis=0)

    dot = functools.partial(jnp.dot, precision=HIGHEST, preferred_element_type=jnp.float32)
    by_inverse = times(inverse[...])
    first, second = sums[:half, :], sums[half : 2 * half, :]
    folded = sums[2 * half :, :]
    one = jnp.concatenate([spread(folded, False), spread(folded, True)], axis=0)
    rest = [spread(first, False), spread(first, True), spread(second, False), spread(second, True)]
    totals = [one] + [value[:n_src] for value in rest]
    totals[-1] = totals[-1] + one
    moves = [times(value[n_src:]) for value in rest]
    coefs = []
    for i, value in enumerate(totals):
        for j in range(i):
            value = value + dot(coefs[j], moves[i - j - 1])
        coefs.append(dot(value, by_inverse))
    sign = lane((n_src, 128)) % 64 < 32
    for i, value in enumerate(coefs):
        coef[:n_src, i * 64 : (i + 1) * 64] = jnp.where(sign, value, -value)[:, :64]
        coef[n_src:, i * 64 : (i + 1) * 64] = pltpu.roll(value, 32, 1)[:, :64]
    turned = coefs[-1].T
    final[0] = turned[:n_coarse]
    final[1] = turned[n_coarse : 2 * n_coarse]


def last_kernel(n_src, *refs):
    *arrived, v1, v2, v3, v4, coef, out, moved, acc = refs
    rows, end = arrived[0].shape
    half = rows // 2
    n_coarse = half - n_src
    for side, value in enumerate(incoming(arrived)):
        cols = slice(side * end, (side + 1) * end)
        for part in range(2):
            base = part * half
            acc[side, part * n_src : (part + 1) * n_src] = value[base : base + n_src]
            moved[part * n_coarse : (part + 1) * n_coarse, cols] = value[base + n_src : base + half]

    def split(value):
        high = value.astype(jnp.bfloat16)
        return high, (value - high.astype(jnp.float32)).astype(jnp.bfloat16)

    left_high, left_low = split(coef[...])
    left = jnp.concatenate([left_high, left_low], axis=0)

    def one(side, carry):
        cols = pl.ds(pl.multiple_of(side * end, 128), end)
        right = jnp.concatenate([ref[:, cols] for ref in (moved, v4, v3, v2, v1)], axis=0)
        high, low = split(right)
        both = jnp.dot(left, high, preferred_element_type=jnp.float32)
        both = both[: 2 * n_src] + both[2 * n_src :]
        acc[side] += both + jnp.dot(left_high, low, preferred_element_type=jnp.float32)
        return carry

    lax.fori_loop(0, 4, one, 0)
    for side in range(4):
        for part in range(2):
            out[part, :, side, :] = acc[side, part * n_src : (part + 1) * n_src]


def per_device(interface_map, source_trace, restriction, prolongation, coarse_inverse):
    _, n_src, _, end = source_trace.shape[2:]
    n_coarse = restriction.shape[3]
    half = n_src + n_coarse
    rows = 2 * half
    f32 = jnp.float32
    lift = prolongation[0, 0]
    table = interface_map[0, 0]
    side = jax.ShapeDtypeStruct((rows, end), f32)
    long_side = jax.ShapeDtypeStruct((rows + 8, end), f32)
    params = pltpu.CompilerParams(vmem_limit_bytes=32 * 1024 * 1024)

    wide = jax.ShapeDtypeStruct((rows, 4 * end), f32)
    *sent, out = pl.pallas_call(
        first_kernel, out_shape=(side, side, long_side, long_side, wide), compiler_params=params, name="first"
    )(source_trace[0, 0], restriction[0, 0])
    src = out
    kept = []
    outs = [out]
    wider = lambda shape: jax.ShapeDtypeStruct((shape.shape[0] + 2 * n_coarse, shape.shape[1]), f32)
    inverse = jnp.concatenate([coarse_inverse[0], coarse_inverse[1]] * 2, axis=1)
    extra_shape = jax.ShapeDtypeStruct((2 * n_coarse, 4 * end), f32)
    for i in range(1, ITERS):
        arrived = exchange(*sent)
        operands = [*arrived] + ([lift] if i == 1 else []) + ([adjoint] if i == 2 else []) + [table, src]
        sides = tuple(wider(x) if i == 2 else x for x in (side, side, long_side, long_side))
        more = {1: (wide, table), 2: (wide,), 3: (wide, extra_shape)}.get(i, ())
        scratch = [pltpu.VMEM((rows, 8 * end), jnp.bfloat16)]
        specs = [pl.BlockSpec(memory_space=pltpu.VMEM)] * len(operands)
        if i == 1:
            specs[-2] = pl.BlockSpec(memory_space=pl.ANY)
            scratch.append(pltpu.SemaphoreType.DMA((4 * end // TILE,)))
        if i > 3:
            scratch.append(pltpu.VMEM((rows, 4 * end), f32))
        out_shape = sides + (extra_shape,) + tuple(jax.ShapeDtypeStruct(x.shape, x.dtype) for x in more)
        results = pl.pallas_call(
            functools.partial(round_kernel, i),
            in_specs=specs,
            out_shape=out_shape,
            scratch_shapes=scratch,
            compiler_params=params,
            cost_estimate=pl.CostEstimate(
                flops=2 * rows * 4 * end * 8 * end, bytes_accessed=12_000_000, transcendentals=0
            ),
            name="round",
        )(*operands)
        sent, extra = results[:4], results[4]
        if i < 4:
            out = results[5]
            outs.append(out)
        if i == 1:
            table = results[6]
        if i == 1:
            seen = extra
            adjoint = pl.pallas_call(
                adjoint_kernel,
                out_shape=extra_shape,
                compiler_params=params,
                cost_estimate=pl.CostEstimate(
                    flops=2 * rows * 4 * end * 8 * end, bytes_accessed=12_000_000, transcendentals=0
                ),
                name="adjoint",
            )(seen, table)
        else:
            kept.append(extra)
        if i == 3:
            t1, t2, t3 = (total(outs[j], seen, seen, params) for j in range(3))
            t45 = total(out, seen, results[6], params)
            at = lane((half, 128)) < 64
            fold = n_src // 2
            folded = jnp.where(lane((fold, 128)) < 64, t1[:fold], t1[fold:n_src])
            sums = butterfly_sum(jnp.concatenate([jnp.where(at, t2, t3), t45, folded], axis=0))
    arrived = exchange(*sent)
    coef, coef_now = pl.pallas_call(
        functools.partial(coef_kernel, n_src),
        out_shape=(
            jax.ShapeDtypeStruct((2 * n_src, (ITERS - 1) * 64), f32),
            jax.ShapeDtypeStruct((2, n_coarse, n_src), f32),
        ),
        compiler_params=params,
        name="coef",
    )(sums, inverse)
    traces = pl.pallas_call(
        functools.partial(last_kernel, n_src),
        out_shape=jax.ShapeDtypeStruct((2, n_src, 4, end), f32),
        scratch_shapes=[pltpu.VMEM((2 * n_coarse, 4 * end), f32), pltpu.VMEM((4, 2 * n_src, end), f32)],
        compiler_params=params,
        name="last",
    )(*arrived, *kept, coef)
    return (traces[None, None], jnp.swapaxes(coef_now, 1, 2))


def total(out, left, right, params):
    return pl.pallas_call(
        total_kernel,
        out_shape=jax.ShapeDtypeStruct((out.shape[0] // 2, 128), jnp.float32),
        compiler_params=params,
        cost_estimate=pl.CostEstimate(flops=300_000_000, bytes_accessed=1_600_000, transcendentals=0),
        name="total",
    )(out, left, right)


def solution(mesh):
    finer = Mesh(
        mesh.devices.reshape(4, 4, mesh.shape["sx"], mesh.shape["wl"]), ("sy_0", "sy_1", "sx", "wl")
    )
    return jax.shard_map(
        per_device,
        mesh=finer,
        in_specs=(
            P(WL_SY, "sx", None, None, None),
            P(WL_SY, "sx", None, None, None, None),
            P(WL_SY, "sx", None, None, None, None),
            P(WL_SY, "sx", None, None, None, None),
            P("wl", None, None),
        ),
        out_specs=(P(WL_SY, "sx", None, None, None, None), P("wl", None, None)),
        check_vma=False,
    )
```

```python
import functools

import jax
import jax.numpy as jnp
from jax import lax
from jax.experimental import pallas as pl
from jax.experimental.pallas import tpu as pltpu
from jax.sharding import Mesh
from jax.sharding import PartitionSpec as P


ITERS = 6
SY = ("sy_0", "sy_1")
WL_SY = ("wl", "sy_0", "sy_1")
HIGHEST = lax.Precision.HIGHEST
TILE = 512
NT = (((1,), (1,)), ((), ()))
SUM_STEPS = (("sy_1", (1, 2, 3)), ("sx", (4,)), ("sy_0", (1, 2, 3)), ("sx", (1, 2, 3)))


def ring(value, axis, by):
    n = lax.axis_size(axis)
    return lax.ppermute(value, axis, [(i, (i + by) % n) for i in range(n)])


def exchange(north, south, west, east):
    from_north = ring(south, SY, 1)
    from_south = ring(north, SY, -1)
    from_west = ring(east, "sx", 1)
    from_east = ring(west, "sx", -1)
    rows = east.shape[0]
    relay = from_north[rows:] + from_south[rows:]
    relay_west = ring(relay, "sx", 1)
    relay_east = ring(relay, "sx", -1)
    return (from_north, from_south, from_west, from_east, relay_west, relay_east)


def butterfly_sum(value):
    for axis, partners in SUM_STEPS:
        n = lax.axis_size(axis)
        others = [lax.ppermute(value, axis, [(i, i ^ p) for i in range(n)]) for p in partners]
        value = functools.reduce(jnp.add, others, value)
    return value


def lane(shape):
    return lax.broadcasted_iota(jnp.int32, shape, 1)


def sublane(shape):
    return lax.broadcasted_iota(jnp.int32, shape, 0)


def write_corners(rows, north, south, west, east):
    end = north.shape[1]
    first = lambda ref: ref[:rows, 0:1]
    last = lambda ref: ref[:rows, end - 1 : end]
    corner_nw = first(north) + first(west)
    corner_ne = last(north) + first(east)
    corner_sw = first(south) + last(west)
    corner_se = last(south) + last(east)
    at = lane((rows, 128))
    zero = jnp.zeros((rows, 128), jnp.float32)
    table = jnp.where(at == 0, corner_se, zero)
    table = jnp.where(at == 1, corner_sw, table)
    table = jnp.where(at == 4, corner_ne, table)
    table = jnp.where(at == 5, corner_nw, table)
    turned = table.T[:8]
    row = sublane((8, rows))
    south[rows:, :] = jnp.zeros((8, end), jnp.float32)
    north[rows:, :] = jnp.zeros((8, end), jnp.float32)
    south[rows:, :rows] = jnp.where(row < 4, turned, 0.0)
    north[rows:, :rows] = jnp.where(row >= 4, turned, 0.0)


def place():
    sy = lax.axis_index("sy_0") * lax.axis_size("sy_1") + lax.axis_index("sy_1")
    sx = lax.axis_index("sx")
    return (
        sy > 0,
        sy < lax.axis_size("sy_0") * lax.axis_size("sy_1") - 1,
        sx > 0,
        sx < lax.axis_size("sx") - 1,
    )


def keep(cond, value):
    return jnp.where(cond, value, jnp.zeros_like(value))


def incoming(refs):
    from_north, from_south, from_west, from_east, relay_west, relay_east = refs
    rows, end = from_west.shape
    has_north, has_south, has_west, has_east = place()
    row = sublane((8, 256))
    mixed = jnp.where(row % 4 == 0, relay_west[:, :256], relay_east[:, :256])
    mixed = jnp.concatenate([mixed, jnp.zeros((120, 256), jnp.float32)], axis=0)
    turned = 0.5 * mixed.T[:rows]
    into_nw = keep(jnp.logical_and(has_north, has_west), turned[:, 0:1])
    into_ne = keep(jnp.logical_and(has_north, has_east), turned[:, 1:2])
    into_sw = keep(jnp.logical_and(has_south, has_west), turned[:, 4:5])
    into_se = keep(jnp.logical_and(has_south, has_east), turned[:, 5:6])
    at = lane((rows, end))

    def side(ref, has, at_first, at_last):
        value = keep(has, ref[:rows, :])
        return value + jnp.where(at == 0, at_first, jnp.where(at == end - 1, at_last, 0.0))

    return (
        side(from_north, has_north, into_nw, into_ne),
        side(from_south, has_south, into_sw, into_se),
        side(from_west, has_west, into_nw, into_sw),
        side(from_east, has_east, into_ne, into_se),
    )


def first_kernel(src, weights, north, south, west, east, whole_out):
    n_src, n_coarse = src.shape[1], weights.shape[1]
    half = n_src + n_coarse
    for side, ref in enumerate((north, south, west, east)):
        for part in range(2):
            ref[part * half : part * half + n_src, :] = src[part, :, side, :]
            ref[part * half + n_src : (part + 1) * half, :] = weights[part, :, side, :]
        whole_out[:, side * ref.shape[1] : (side + 1) * ref.shape[1]] = ref[: 2 * half, :]
    write_corners(2 * half, north, south, west, east)


def round_kernel(number, *refs):
    first, sends, receives, hides = number == 1, number == 2, number == 3, number > 3
    arrived, refs = refs[:6], list(refs[6:])
    lift = refs.pop(0) if first else None
    sent_along = refs.pop(0) if sends else None
    far = refs.pop(0) if first else None
    table = None if first else refs.pop(0)
    src, north, south, west, east, extra = refs[:6]
    rest = refs[6:]
    if hides:
        block, whole_out = rest
    elif first:
        whole_out, table, block, arrives = rest
    elif receives:
        whole_out, received, block = rest
    else:
        whole_out, block = rest
    end = arrived[0].shape[1]
    rows = whole_out.shape[0]
    half = rows // 2
    n_src = half - extra.shape[0] // 2
    count = 4 * end // TILE

    def bring(t):
        cols = pl.ds(pl.multiple_of(t * TILE, TILE), TILE)
        return pltpu.make_async_copy(far.at[:, :, cols], table.at[:, :, cols], arrives.at[t])

    if first:
        for t in range(count):
            bring(t).start()
    n_coarse = half - n_src
    row, col = sublane((256, 256)), lane((256, 256))
    weave = (row == col // 2 + 128 * (col % 2)).astype(jnp.bfloat16)
    for side, value in enumerate(incoming(arrived)):
        cols = slice(side * end, (side + 1) * end)
        if receives:
            received[:, cols] = value[rows:]
        plain = []
        for part in range(2):
            base = part * half
            extra[part * n_coarse : (part + 1) * n_coarse, cols] = value[base + n_src : base + half]
            low = value[base : base + n_src].astype(jnp.bfloat16)
            if first:
                high = lift[part, :, side, :].astype(jnp.bfloat16)
            else:
                high = value[base + n_src : base + half].astype(jnp.bfloat16)
            plain.append(jnp.concatenate([low, high], axis=0))
        straight = jnp.concatenate(plain, axis=0)
        turned = jnp.concatenate([-plain[1], plain[0]], axis=0)
        for k in range(0, end, 128):
            pair = jnp.concatenate([straight[:, k : k + 128], turned[:, k : k + 128]], axis=1)
            woven = jnp.dot(pair, weave, preferred_element_type=jnp.float32)
            block[:, 2 * (side * end + k) : 2 * (side * end + k) + 256] = woven.astype(jnp.bfloat16)

    def columns(t, carry):
        cols = pl.ds(pl.multiple_of(t * TILE, TILE), TILE)
        if first:
            bring(t).wait()
        whole_out[:, cols] = jnp.dot(
            block[...], table[:, :, cols].reshape(8 * end, TILE), preferred_element_type=jnp.float32
        )
        return carry

    lax.fori_loop(0, count, columns, 0)
    for side, ref in enumerate((north, south, west, east)):
        cols = slice(side * end, (side + 1) * end)
        for part in range(2):
            base = part * half
            value = whole_out[base : base + n_src, cols] + src[base : base + n_src, cols]
            ref[base : base + n_src, :] = value
            if not hides:
                whole_out[base : base + n_src, cols] = value
            ref[base + n_src : base + half, :] = whole_out[base + n_src : base + half, cols]
        if sends:
            ref[rows : west.shape[0], :] = sent_along[:, cols]
    write_corners(west.shape[0], north, south, west, east)


def adjoint_kernel(weights, table, out):
    n, length = weights.shape
    half = n // 2
    value = weights[...]
    high = value.astype(jnp.bfloat16)
    low = (value - high.astype(jnp.float32)).astype(jnp.bfloat16)
    left = jnp.concatenate([high, low], axis=0)
    row, col = sublane((256, 256)), lane((256, 256))
    unweave = (col == row // 2 + 128 * (row % 2)).astype(jnp.bfloat16)

    def some(t, carry):
        for k in range(3):
            here = pl.multiple_of(t * 384 + k * 128, 128)
            part = table[pl.ds(here, 128), :, :].reshape(256, length)
            both = lax.dot_general(left, part, NT, preferred_element_type=jnp.float32)
            both = both[:n] + both[n:]
            upper = both.astype(jnp.bfloat16)
            rest = both - upper.astype(jnp.float32)
            middle = rest.astype(jnp.bfloat16)
            lower = (rest - middle.astype(jnp.float32)).astype(jnp.bfloat16)
            split = jnp.concatenate([upper, middle, lower], axis=0)
            split = jnp.dot(split, unweave, preferred_element_type=jnp.float32)
            both = split[:n] + split[n : 2 * n] + split[2 * n :]
            out[:half, pl.ds(here, 128)] = both[:half, :128] - both[half:, 128:]
            out[half:, pl.ds(here, 128)] = both[:half, 128:] + both[half:, :128]
        return carry

    lax.fori_loop(0, length // 384, some, 0)


def total_kernel(out, left, right, total):
    rows, length = out.shape
    half = rows // 2

    def columns(t, acc):
        cols = pl.ds(pl.multiple_of(t * TILE, TILE), TILE)
        return acc + lax.dot_general(
            out[:, cols],
            jnp.concatenate([left[:, cols], right[:, cols]], axis=0),
            NT,
            precision=HIGHEST,
            preferred_element_type=jnp.float32,
        )

    acc = lax.fori_loop(0, length // TILE, columns, jnp.zeros((rows, 128), jnp.float32))
    at = lane((half, 128)) % 64 < 32
    ahead, behind = pltpu.roll(acc[half:], 96, 1), pltpu.roll(acc[half:], 32, 1)
    total[...] = acc[:half] + jnp.where(at, -ahead, behind)


def coef_kernel(n_src, sums, inverse, coef, final):
    n_coarse = inverse.shape[0]
    half = n_src + n_coarse

    def spread(value, upper):
        at = lane(value.shape) >= 64
        kept = jnp.where(at if upper else jnp.logical_not(at), value, 0.0)
        return kept + pltpu.roll(kept, 64, 1)

    def times(value):
        sign = lane((n_coarse, 128)) % 64 < 32
        moved = pltpu.roll(value, 32, 1)
        lower = jnp.where(sign, -moved, moved)
        return jnp.concatenate([value, lower, jnp.zeros((128 - 2 * n_coarse, 128), jnp.float32)], axis=0)

    dot = functools.partial(jnp.dot, precision=HIGHEST, preferred_element_type=jnp.float32)
    by_inverse = times(inverse[...])
    first, second = sums[:half, :], sums[half : 2 * half, :]
    folded = sums[2 * half :, :]
    one = jnp.concatenate([spread(folded, False), spread(folded, True)], axis=0)
    rest = [spread(first, False), spread(first, True), spread(second, False), spread(second, True)]
    totals = [one] + [value[:n_src] for value in rest]
    totals[-1] = totals[-1] + one
    moves = [times(value[n_src:]) for value in rest]
    coefs = []
    for i, value in enumerate(totals):
        for j in range(i):
            value = value + dot(coefs[j], moves[i - j - 1])
        coefs.append(dot(value, by_inverse))
    sign = lane((n_src, 128)) % 64 < 32
    for i, value in enumerate(coefs):
        coef[:n_src, i * 64 : (i + 1) * 64] = jnp.where(sign, value, -value)[:, :64]
        coef[n_src:, i * 64 : (i + 1) * 64] = pltpu.roll(value, 32, 1)[:, :64]
    turned = coefs[-1].T
    final[0] = turned[:n_coarse]
    final[1] = turned[n_coarse : 2 * n_coarse]


def last_kernel(n_src, *refs):
    *arrived, v1, v2, v3, v4, coef, out, moved, acc = refs
    rows, end = arrived[2].shape
    half = rows // 2
    n_coarse = half - n_src
    for side, value in enumerate(incoming(arrived)):
        cols = slice(side * end, (side + 1) * end)
        for part in range(2):
            base = part * half
            acc[side, part * n_src : (part + 1) * n_src] = value[base : base + n_src]
            moved[part * n_coarse : (part + 1) * n_coarse, cols] = value[base + n_src : base + half]

    def split(value):
        high = value.astype(jnp.bfloat16)
        return high, (value - high.astype(jnp.float32)).astype(jnp.bfloat16)

    left_high, left_low = split(coef[...])
    left = jnp.concatenate([left_high, left_low], axis=0)

    def one(side, carry):
        cols = pl.ds(pl.multiple_of(side * end, 128), end)
        right = jnp.concatenate([ref[:, cols] for ref in (moved, v4, v3, v2, v1)], axis=0)
        high, low = split(right)
        both = jnp.dot(left, high, preferred_element_type=jnp.float32)
        both = both[: 2 * n_src] + both[2 * n_src :]
        acc[side] += both + jnp.dot(left_high, low, preferred_element_type=jnp.float32)
        return carry

    lax.fori_loop(0, 4, one, 0)
    for side in range(4):
        for part in range(2):
            out[part, :, side, :] = acc[side, part * n_src : (part + 1) * n_src]


def per_device(interface_map, source_trace, restriction, prolongation, coarse_inverse):
    _, n_src, _, end = source_trace.shape[2:]
    n_coarse = restriction.shape[3]
    half = n_src + n_coarse
    rows = 2 * half
    f32 = jnp.float32
    lift = prolongation[0, 0]
    table = interface_map[0, 0]
    side = jax.ShapeDtypeStruct((rows, end), f32)
    long_side = jax.ShapeDtypeStruct((rows + 8, end), f32)
    params = pltpu.CompilerParams(vmem_limit_bytes=32 * 1024 * 1024)

    wide = jax.ShapeDtypeStruct((rows, 4 * end), f32)
    *sent, out = pl.pallas_call(
        first_kernel, out_shape=(long_side, long_side, side, side, wide), compiler_params=params, name="first"
    )(source_trace[0, 0], restriction[0, 0])
    src = out
    kept = []
    outs = [out]
    wider = lambda shape: jax.ShapeDtypeStruct((shape.shape[0] + 2 * n_coarse, shape.shape[1]), f32)
    inverse = jnp.concatenate([coarse_inverse[0], coarse_inverse[1]] * 2, axis=1)
    extra_shape = jax.ShapeDtypeStruct((2 * n_coarse, 4 * end), f32)
    for i in range(1, ITERS):
        arrived = exchange(*sent)
        operands = [*arrived] + ([lift] if i == 1 else []) + ([adjoint] if i == 2 else []) + [table, src]
        sides = tuple(wider(x) if i == 2 else x for x in (long_side, long_side, side, side))
        more = {1: (wide, table), 2: (wide,), 3: (wide, extra_shape)}.get(i, ())
        scratch = [pltpu.VMEM((rows, 8 * end), jnp.bfloat16)]
        specs = [pl.BlockSpec(memory_space=pltpu.VMEM)] * len(operands)
        if i == 1:
            specs[-2] = pl.BlockSpec(memory_space=pl.ANY)
            scratch.append(pltpu.SemaphoreType.DMA((4 * end // TILE,)))
        if i > 3:
            scratch.append(pltpu.VMEM((rows, 4 * end), f32))
        out_shape = sides + (extra_shape,) + tuple(jax.ShapeDtypeStruct(x.shape, x.dtype) for x in more)
        results = pl.pallas_call(
            functools.partial(round_kernel, i),
            in_specs=specs,
            out_shape=out_shape,
            scratch_shapes=scratch,
            compiler_params=params,
            cost_estimate=pl.CostEstimate(
                flops=2 * rows * 4 * end * 8 * end, bytes_accessed=12_000_000, transcendentals=0
            ),
            name="round",
        )(*operands)
        sent, extra = results[:4], results[4]
        if i < 4:
            out = results[5]
            outs.append(out)
        if i == 1:
            table = results[6]
        if i == 1:
            seen = extra
            adjoint = pl.pallas_call(
                adjoint_kernel,
                out_shape=extra_shape,
                compiler_params=params,
                cost_estimate=pl.CostEstimate(
                    flops=2 * rows * 4 * end * 8 * end, bytes_accessed=12_000_000, transcendentals=0
                ),
                name="adjoint",
            )(seen, table)
        else:
            kept.append(extra)
        if i == 3:
            t1, t2, t3 = (total(outs[j], seen, seen, params) for j in range(3))
            t45 = total(out, seen, results[6], params)
            at = lane((half, 128)) < 64
            fold = n_src // 2
            folded = jnp.where(lane((fold, 128)) < 64, t1[:fold], t1[fold:n_src])
            sums = butterfly_sum(jnp.concatenate([jnp.where(at, t2, t3), t45, folded], axis=0))
    arrived = exchange(*sent)
    coef, coef_now = pl.pallas_call(
        functools.partial(coef_kernel, n_src),
        out_shape=(
            jax.ShapeDtypeStruct((2 * n_src, (ITERS - 1) * 64), f32),
            jax.ShapeDtypeStruct((2, n_coarse, n_src), f32),
        ),
        compiler_params=params,
        name="coef",
    )(sums, inverse)
    traces = pl.pallas_call(
        functools.partial(last_kernel, n_src),
        out_shape=jax.ShapeDtypeStruct((2, n_src, 4, end), f32),
        scratch_shapes=[pltpu.VMEM((2 * n_coarse, 4 * end), f32), pltpu.VMEM((4, 2 * n_src, end), f32)],
        compiler_params=params,
        name="last",
    )(*arrived, *kept, coef)
    return (traces[None, None], jnp.swapaxes(coef_now, 1, 2))


def total(out, left, right, params):
    return pl.pallas_call(
        total_kernel,
        out_shape=jax.ShapeDtypeStruct((out.shape[0] // 2, 128), jnp.float32),
        compiler_params=params,
        cost_estimate=pl.CostEstimate(flops=300_000_000, bytes_accessed=1_600_000, transcendentals=0),
        name="total",
    )(out, left, right)


def solution(mesh):
    finer = Mesh(
        mesh.devices.reshape(4, 4, mesh.shape["sx"], mesh.shape["wl"]), ("sy_0", "sy_1", "sx", "wl")
    )
    return jax.shard_map(
        per_device,
        mesh=finer,
        in_specs=(
            P(WL_SY, "sx", None, None, None),
            P(WL_SY, "sx", None, None, None, None),
            P(WL_SY, "sx", None, None, None, None),
            P(WL_SY, "sx", None, None, None, None),
            P("wl", None, None),
        ),
        out_specs=(P(WL_SY, "sx", None, None, None, None), P("wl", None, None)),
        check_vma=False,
    )
```
